32 devices in a mesh: gx: 4 (over y, core), gy: 4 (over z), gz: 2 (over x).
Axes of the slice: x: 2, y: 2, z: 4, core: 2. Of those that a mesh axis runs over, the one named last changes fastest.
Arguments:
- inputs: bfloat16 [32768, 2048], P(('gx', 'gy', 'gz')), may hold values from -6 to 6
- cotangent: bfloat16 [32768, 4096], P(('gx', 'gy', 'gz')), may hold values from -0.032958984 to 0.032958984
- master: float32 [2048, 4096], P(('gx', 'gy', 'gz')), may hold values from -3 to 3
- accum: float32 [2048, 4096], P(('gx', 'gy', 'gz')), may hold values from 0.05 to 1
Outputs:
- new_master: float32 [2048, 4096], P(('gx', 'gy', 'gz'))
- new_accum: float32 [2048, 4096], P(('gx', 'gy', 'gz'))
The draws below stay inside these ranges and needn't reach their ends.
All inputs are finite; a program needn't handle non-finite values.
Results may differ from the reference program's by a relative error of at most 0.0003.
Values sent between devices are 32-bit elements; how exact they have to be, the bound alone decides.
A program may use at most 128 MiB of HBM per device.

```python
import math
import jax
import jax.numpy as jnp
from jax import lax

D = 4096
ROWS = 2048
TOKENS = 32768


def spiked(drawn, rng, source, target, shards_of, factor):
    owner, partner = [(jnp.arange(drawn.shape[position]) // (drawn.shape[position] // shards_of)).reshape([-1 if axis == position else 1 for axis in range(drawn.ndim)]) for position in (source, target)]
    chosen = jax.random.permutation(rng, shards_of)[partner]
    strong = (owner == chosen) | (owner == (partner + shards_of // 2) % shards_of)
    return jnp.where(strong, factor * drawn, drawn)


def shard_levels(rng, shape, shards, low, high):
    factor_of, own = 1.0, jax.random.fold_in(rng, 6)
    for axis_at, parts in shards:
        steps = jnp.exp(jax.random.uniform(jax.random.fold_in(own, axis_at), (parts,), jnp.float32, low / len(shards), high / len(shards)))
        factor_of = factor_of * jnp.repeat(steps, shape[axis_at] // parts).reshape([-1 if axis == axis_at else 1 for axis in range(len(shape))])
    return factor_of


def bell_draw(stream_key, dims, spread, most, cuts=(), dtype=jnp.bfloat16):
    array = spread * jax.random.normal(stream_key, dims, jnp.float32)
    if cuts:
        array = array * shard_levels(stream_key, dims, cuts, -0.22, 0.18)
    return jnp.clip(array, -most, most).astype(dtype)


def heavy_noise(own_key, dims, width, most, split, heavy, dtype=jnp.bfloat16):
    values = width * jax.random.normal(own_key, dims, jnp.float32)
    if split:
        values = values * shard_levels(own_key, dims, split, -0.22, 0.18)
    return jnp.clip(spiked(values, jax.random.fold_in(own_key, 3), *heavy), -most, most).astype(dtype)


def setup_inputs(seed: int = 0) -> dict:
    key_list = jax.random.split(jax.random.key(seed), 5)
    return {
        "inputs": heavy_noise(key_list[0], (TOKENS, ROWS), 1.0, 6.0, ((0, 32),), (0, 1, 32, 2.75)),
        "cotangent": bell_draw(key_list[1], (TOKENS, D), (TOKENS ** -0.5), 0.032958984, ((0, 32),)),
        "master": bell_draw(key_list[2], (ROWS, D), 0.5, 3.0, ((0, 32),), jnp.float32),
        "accum": jnp.clip(jnp.exp(math.log(1.0) - 2.9957323 * jax.random.uniform(key_list[3], (ROWS, D), jnp.float32) ** shard_levels(key_list[3], (ROWS, D), ((0, 32),), -0.2, 0.2)), 0.05, 1.0),
    }


def reference(inputs, cotangent, master, accum):
    gradient = lax.dot_general(inputs, cotangent, (((0,), (0,)), ((), ())), preferred_element_type=jnp.float32)
    squares = jnp.sum(gradient * gradient)
    limit = 0.5 * jnp.sqrt(jnp.float32(ROWS * D))
    factor = limit / jnp.maximum(jnp.sqrt(squares), limit)
    scaled = factor * gradient
    new_accum = accum + scaled * scaled
    new_master = master - 0.5 * scaled / jnp.sqrt(new_accum)
    return (new_master, new_accum)
```

```python
import functools
import math

import jax
import jax.numpy as jnp
from jax import lax
from jax.experimental import pallas as pl
from jax.experimental.pallas import tpu as pltpu
from jax.sharding import PartitionSpec as P

AXES = ("gx", "gy", "gz")
MESH = pl.DeviceIdType.MESH
PATTERN = "XYZXYUXYXYZXYUXY"


def bits_of(n):
    return n.bit_length() - 1


def plan(sizes):
    bits = [(a, 1 << b) for a, n in zip(AXES, sizes) for b in reversed(range(bits_of(n)))]
    core = bits.index(("gx", 1))
    ys = [i for i, (a, w) in enumerate(bits) if a == "gx" and w > 1]
    zs = [i for i, (a, w) in enumerate(bits) if a == "gy"][::-1]
    xs = [i for i, (a, w) in enumerate(bits) if a == "gz"][::-1]
    orders = {
        "X": xs + ys + zs,
        "Y": ys + xs + zs,
        "Z": zs[:1] + xs + ys + zs[1:],
        "U": zs[:1] + ys + xs + zs[1:],
    }
    return bits, core, orders


def events(bits, orders, pieces):
    free, ready, out = {}, [], []
    for k in range(len(pieces)):
        ready.append((k + 1.0, 0, k))
    while ready:
        ready.sort()
        at, phase, k = ready.pop(0)
        out.append((phase, k))
        order = orders[pieces[k]]
        if phase < len(order):
            link = bits[order[phase]]
            cost = 6.0 / (1 << phase) * (2 if link[1] > 1 and link[0] == "gy" else 1)
            free[link] = max(free.get(link, 0.0), at) + cost
            ready.append((free[link] + 1.5, phase + 1, k))
    return out


def kernel(sizes, pieces, rows, width, *refs):
    bits, core, orders = plan(sizes)
    nb = len(bits)
    rest = [i for i in range(nb) if i != core]
    p_ref, grad_ref, total_ref, own = refs[:4]
    recv = refs[4 : 4 + nb]
    mine, got, own_sem, send_sem, recv_sem, tot_send, tot_recv = refs[4 + nb :]
    here = {a: lax.axis_index(a) for a in AXES}
    at = [lax.rem(here[a] // w, 2) for a, w in bits]

    def partner(i):
        a, w = bits[i]
        return {a: here[a] + w - 2 * w * at[i]}

    peers = [
        [{a: lax.rem(here[a] + k, n)} for k in range(1, n)] for a, n in zip(AXES, sizes)
    ]
    barrier = pltpu.get_barrier_semaphore()
    for row in peers:
        for peer in row:
            pl.semaphore_signal(barrier, inc=1, device_id=peer, device_id_type=MESH)
    pl.semaphore_wait(barrier, sum(len(row) for row in peers))

    step = width // len(pieces)

    def source(k, which):
        index = tuple(which if i == core else slice(None) for i in range(nb))
        return p_ref.at[index + (slice(None), pl.ds(k * step, step))]

    def local(k):
        return pltpu.make_async_copy(source(k, at[core]), own.at[k], own_sem.at[k])

    def view(k, chosen):
        return own.at[(k,) + tuple(chosen.get(i, slice(None)) for i in rest)]

    def remote(phase, k):
        if phase == 0:
            src, i = source(k, 1 - at[core]), core
        else:
            order = orders[pieces[k]]
            i = order[phase - 1]
            chosen = {j: at[j] for j in order[: phase - 1]}
            chosen[i] = 1 - at[i]
            src = view(k, chosen)
        return pltpu.make_async_remote_copy(
            src_ref=src,
            dst_ref=recv[phase].at[k],
            send_sem=send_sem.at[phase, k],
            recv_sem=recv_sem.at[phase, k],
            device_id=partner(i),
            device_id_type=MESH,
        )

    def add(phase, k, fixed=None):
        done = orders[pieces[k]][:phase]
        open_bits = [i for i in rest if i not in done]
        loop_bits = [i for i in open_bits if fixed is None or i != fixed[0]]

        def body(n, carry):
            value = {i: lax.rem(n // (1 << j), 2) for j, i in enumerate(loop_bits)}
            if fixed is not None:
                value[fixed[0]] = fixed[1]
            place = (k,) + tuple(value.get(i, at[i]) for i in rest)
            inner = (k,) + tuple(value[i] for i in open_bits)
            own[place] = own[place] + recv[phase][inner]
            return carry

        lax.fori_loop(0, 1 << len(loop_bits), body, 0)

    for k in range(len(pieces)):
        remote(0, k).start()
        local(k).start()
    squares = jnp.zeros((8, 128), jnp.float32)
    for phase, k in events(bits, orders, pieces):
        remote(phase, k).wait_recv()
        if phase == 0:
            local(k).wait()
        if phase < nb - 1:
            i = orders[pieces[k]][phase]
            add(phase, k, (i, 1 - at[i]))
            remote(phase + 1, k).start()
            add(phase, k, (i, at[i]))
        else:
            place = (k,) + tuple(at[i] for i in rest)
            block = own[place] + recv[phase][k]
            grad_ref[:, k * step : (k + 1) * step] = block
            square = block * block
            square = jnp.sum(square.reshape(rows // 8, 8, step), axis=0)
            for c in range(step // 128):
                squares = squares + square[:, c * 128 : (c + 1) * 128]
    slot = 0
    value = jnp.broadcast_to(jnp.sum(squares, keepdims=True), (8, 128))
    for stage, row in enumerate(peers):
        mine[stage] = value
        copies = []
        for peer in row:
            copy = pltpu.make_async_remote_copy(
                src_ref=mine.at[stage],
                dst_ref=got.at[slot],
                send_sem=tot_send.at[slot],
                recv_sem=tot_recv.at[slot],
                device_id=peer,
                device_id_type=MESH,
            )
            copy.start()
            copies.append((copy, slot))
            slot += 1
        for copy, place in copies:
            copy.wait()
            value = value + got[place]
    total_ref[...] = value
    for phase in range(nb):
        for k in range(len(pieces)):
            remote(phase, k).wait_send()


def reduce_gradient(partial, sizes, rows, width):
    bits, core, orders = plan(sizes)
    nb = len(bits)
    pieces = PATTERN
    step = width // len(pieces)
    slots = sum(n - 1 for n in sizes)
    vmem = lambda *shape: pltpu.VMEM(shape, jnp.float32)
    dma = lambda *shape: pltpu.SemaphoreType.DMA(shape)
    return pl.pallas_call(
        functools.partial(kernel, sizes, pieces, rows, width),
        out_shape=(
            jax.ShapeDtypeStruct((rows, width), jnp.float32),
            jax.ShapeDtypeStruct((8, 128), jnp.float32),
        ),
        in_specs=[pl.BlockSpec(memory_space=pl.ANY)],
        out_specs=(pl.BlockSpec(memory_space=pltpu.VMEM),) * 2,
        scratch_shapes=[
            vmem(len(pieces), *[2] * (nb - 1), rows, step),
            *[vmem(len(pieces), *[2] * (nb - 1 - p), rows, step) for p in range(nb)],
            vmem(len(sizes), 8, 128),
            vmem(slots, 8, 128),
            dma(len(pieces)),
            dma(nb, len(pieces)),
            dma(nb, len(pieces)),
            dma(slots),
            dma(slots),
        ],
        compiler_params=pltpu.CompilerParams(
            collective_id=0, has_side_effects=True, vmem_limit_bytes=60 << 20
        ),
    )(partial.reshape([2] * nb + [rows, width]))


def shards(sizes, inputs, cotangent, master, accum):
    rows, width = master.shape
    partial = lax.dot_general(
        inputs, cotangent, (((0,), (0,)), ((), ())), preferred_element_type=jnp.float32
    )
    gradient, total = reduce_gradient(partial, sizes, rows, width)
    squares = total[0, 0]
    limit = 0.5 * jnp.sqrt(jnp.float32(rows * math.prod(sizes) * width))
    factor = limit / jnp.maximum(jnp.sqrt(squares), limit)
    scaled = factor * gradient
    new_accum = accum + scaled * scaled
    new_master = master - 0.5 * scaled / jnp.sqrt(new_accum)
    return (new_master, new_accum)


def solution(mesh):
    sizes = tuple(mesh.shape[a] for a in AXES)
    spec = P(AXES, None)
    return jax.shard_map(
        functools.partial(shards, sizes),
        mesh=mesh,
        in_specs=(spec,) * 4,
        out_specs=(spec, spec),
        check_vma=False,
    )
```
